32 devices in a mesh: dev: 32 (over z, y, x, core).
Axes of the slice: x: 2, y: 2, z: 4, core: 2. Of those that a mesh axis runs over, the one named last changes fastest.
Arguments:
- state: float32 [128, 512, 128], P('dev'), may hold values from -6 to 6
- background: float32 [128, 512, 128], P('dev'), may hold values from -6 to 6
- back_precision: float32 [128], replicated, may hold values from 0.2 to 2
- conv_first: bfloat16 [3, 3, 128, 128], replicated, may hold values from -0.1875 to 0.1875
- bias_first: float32 [128], replicated, may hold values from -3 to 3
- conv_second: bfloat16 [3, 3, 128, 128], replicated, may hold values from -0.1875 to 0.1875
- sounding_tile: int32 [16384, 1], P('dev'), may hold values from 0 to 31; in each aligned block of 512 rows (0 to 511, 512 to 1023, ...) at most 32 rows name the same one
- sounding_cells: int32 [16384, 4], P('dev'), may hold values from 0 to 2047
- cell_weights: float32 [16384, 4], P('dev'), may hold values from 0.1 to 1
- observations: float32 [16384, 616], P('dev'), may hold values from -6 to 6
- live_counts: int32 [32], P('dev'), may hold values from 1 to 511, as said below
- layer_in: bfloat16 [128, 1024], replicated, may hold values from -0.5 to 0.5
- bias_in: float32 [1024], replicated, may hold values from -3 to 3
- layer_out: bfloat16 [1024, 616], replicated, may hold values from -0.1875 to 0.1875
- bias_out: float32 [616], replicated, may hold values from -3 to 3
- error_precision: float32 [616, 616], replicated, as said below
Outputs:
- gradient: float32 [128, 512, 128], P('dev')
The draws below stay inside these ranges and needn't reach their ends.
Inputs may be any that keep to these rules, and one draw needn't show every extreme that they name: `sounding_tile`: among the 512 soundings of one list, at most 32 lie in the same strip, and in some lists some strip holds exactly 32 of them. The live soundings of a list are its first live_counts; the counts of lists l and l + 16 sum to 512. `error_precision`: Symmetric.
All inputs are finite; a program needn't handle non-finite values.
Results may differ from the reference program's by a relative error of at most 0.008.
Values may be sent and summed in bfloat16 or wider, within the bound.
A program may use at most 64 MiB of HBM per device.

```python
import math
import jax
import jax.numpy as jnp
import numpy as np
from jax import lax

CH = 128
HID = 1024
NCHAN = 616
NCOLS = 512
MARGIN = 4
ROWS_DEV = 4
SND_DEV = 512
LISTS = 32
NROWS = 128
SOUNDINGS = 16384
CAP = 32
N_DEV = 32


def draw_live_counts(key, part):
    half_lists = LISTS // 2
    first_half = jax.random.randint(key, (half_lists,), 1, SND_DEV, dtype=jnp.int32)
    return jnp.concatenate([first_half, SND_DEV - first_half])


def draw_error_precision(key, part):
    key_off, key_diag = jax.random.split(jax.random.fold_in(key, 17))
    draws_raw = jax.random.normal(key_off, (NCHAN, NCHAN), jnp.float32)
    off_part = (draws_raw + draws_raw.T) * (0.35 / math.sqrt(NCHAN))
    diagonal = jax.random.uniform(key_diag, (NCHAN,), jnp.float32, 1.0, 3.0)
    return off_part + jnp.diag(diagonal)


def plant(drawn, own_key, low, largest):
    index_at = [jax.random.randint(jax.random.fold_in(own_key, axis), (), 0, length) for axis, length in enumerate(drawn.shape)]
    main_axis = drawn.shape.index(max(drawn.shape))
    beside = index_at[:main_axis] + [(index_at[main_axis] + 1) % drawn.shape[main_axis]] + index_at[main_axis + 1:]
    return drawn.at[tuple(index_at)].set(low).at[tuple(beside)].set(largest)


def level_of(rng, shape, cuts, low, high):
    def one(axis_at, blocks):
        steps = jax.random.uniform(jax.random.fold_in(jax.random.fold_in(rng, 6), axis_at), (blocks,), jnp.float32, low / len(cuts), high / len(cuts))
        return jnp.repeat(jnp.exp(steps), shape[axis_at] // blocks).reshape((-1,) + (1,) * (len(shape) - axis_at - 1))

    factor_of = one(*cuts[0])
    for cut in cuts[1:]:
        factor_of = factor_of * one(*cut)
    return factor_of


def routed_block(key, own, number, rows, count, top, most, slope):
    order = jax.random.permutation(key, count)
    crowded, ordinary = portions_of(count, rows * top, most, slope, True), portions_of(count, rows * top, most, slope, False)
    places = jnp.arange(count)

    def named(sizes, rotation):
        used = int((sizes > 0).sum())
        fixed = max(1, used // 4)
        moved = fixed + (places - fixed + rotation * (used - fixed)) % max(1, count - fixed)
        return jnp.zeros((count,), jnp.int32).at[order[jnp.where(places < fixed, places, moved)]].set(jnp.asarray(sizes, jnp.int32))

    sizes = jnp.where(number % 4 == 0, named(crowded, number // 4), named(ordinary, number - number // 4 - 1))
    mixed = jax.random.permutation(jax.random.fold_in(own, 3), count)
    donor, receiver = mixed[0:count // 2 * 2:2], mixed[1:count // 2 * 2:2]
    margin = jnp.minimum(sizes[donor] - 1, most - sizes[receiver]) // 2
    margin = jnp.where((donor == order[0]) | (receiver == order[0]) | (sizes[receiver] == 0), 0, jnp.maximum(margin, 0))
    moved = jax.random.randint(jax.random.fold_in(own, 4), (count // 2,), 0, 1 << 20) % (margin + 1)
    sizes = sizes.at[donor].add(-moved).at[receiver].add(moved)
    items = jnp.searchsorted(jnp.cumsum(sizes), jnp.arange(rows * top), side="right").astype(jnp.int32)
    listing = items.reshape(top, rows).T
    listing = listing[jax.random.permutation(jax.random.fold_in(own, 1), rows)]
    rotation = jax.random.randint(jax.random.fold_in(own, 2), (rows, 1), 0, top)
    return jnp.take_along_axis(listing, (jnp.arange(top)[None, :] + rotation) % top, axis=1)


def portions_of(amount, total, reach, lean, full):
    portions = [(1 << 20) // math.isqrt(standing ** lean) + 1 for standing in range(1, amount + 1)]
    largest = reach if full else min(reach, max(-(-total // amount), total * portions[0] // sum(portions)))
    least = 1 if total - largest >= amount - 1 else 0
    holding, spare = [largest] + [least] * (amount - 1), total - largest - least * (amount - 1)
    while spare > 0:
        movable = [i for i in range(1, amount) if holding[i] < largest] or [i for i in range(1, amount) if holding[i] < reach]
        pool, left = sum([portions[i] for i in movable]), spare
        for i in movable:
            more = min(reach - holding[i], max(1, left * portions[i] // pool), spare)
            holding[i] = holding[i] + more
            spare = spare - more
    return np.array(holding)


def bell_draw(rng, dims, deviation, bound, pieces=(), held_as=jnp.bfloat16):
    array = jax.random.normal(rng, dims, jnp.float32) * deviation
    if len(pieces) > 0:
        array = level_of(rng, dims, pieces, -0.22, 0.18) * array
    return jnp.clip(array, min=-bound, max=bound).astype(held_as)


def setup_inputs(seed: int = 0) -> dict:
    key_list = jax.random.split(jax.random.key(seed), 17)
    state = bell_draw(key_list[0], (NROWS, NCOLS, CH), 1.0, 6.0, ((0, 32),), jnp.float32)
    background = bell_draw(key_list[1], (NROWS, NCOLS, CH), 1.0, 6.0, ((0, 32),), jnp.float32)
    back_precision = jnp.clip(jnp.exp(jax.random.uniform(key_list[2], (CH,), jnp.float32, math.log(0.2), math.log(2.0))), 0.2, 2.0)
    conv_first = bell_draw(key_list[3], (3, 3, CH, CH), (9 * CH) ** -0.5, 0.1875)
    bias_first = bell_draw(key_list[4], (CH,), 0.5, 3.0, (), jnp.float32)
    conv_second = bell_draw(key_list[5], (3, 3, CH, CH), (9 * CH) ** -0.5, 0.1875)
    sounding_tile_keys = jax.random.split(jax.random.fold_in(key_list[6], 1), SOUNDINGS // SND_DEV)
    sounding_tile_turns = jax.random.permutation(jax.random.fold_in(key_list[6], 3), SOUNDINGS // SND_DEV)
    sounding_tile = jax.vmap(lambda own, number: routed_block(jax.random.fold_in(key_list[6], 2), own, number, SND_DEV, LISTS, 1, CAP, 2))(sounding_tile_keys, sounding_tile_turns).reshape((SOUNDINGS, 1))
    sounding_cells = plant(jax.random.randint(key_list[7], (SOUNDINGS, MARGIN), 0, ROWS_DEV * NCOLS), jax.random.fold_in(key_list[7], 1), 0, (ROWS_DEV * NCOLS) - 1).astype(jnp.int32)
    cell_weights = jnp.clip(jnp.exp(math.log(1.0) - 2.3025851 * jax.random.uniform(key_list[8], (SOUNDINGS, MARGIN), jnp.float32) ** level_of(key_list[8], (SOUNDINGS, MARGIN), ((0, 32),), -0.2, 0.2)), 0.1, 1.0)
    observations = bell_draw(key_list[9], (SOUNDINGS, NCHAN), 1.0, 6.0, ((0, 32),), jnp.float32)
    live_counts = draw_live_counts(jax.random.fold_in(key_list[16], 71), 0)
    layer_in = bell_draw(key_list[11], (CH, HID), CH ** -0.5, 0.5)
    bias_in = bell_draw(key_list[12], (HID,), 0.5, 3.0, (), jnp.float32)
    layer_out = bell_draw(key_list[13], (HID, NCHAN), HID ** -0.5, 0.1875)
    bias_out = bell_draw(key_list[14], (NCHAN,), 0.5, 3.0, (), jnp.float32)
    error_precision = draw_error_precision(jax.random.fold_in(key_list[16], 71), 0)
    return dict(state=state, background=background, back_precision=back_precision, conv_first=conv_first, bias_first=bias_first, conv_second=conv_second, sounding_tile=sounding_tile, sounding_cells=sounding_cells, cell_weights=cell_weights, observations=observations, live_counts=live_counts, layer_in=layer_in, bias_in=bias_in, layer_out=layer_out, bias_out=bias_out, error_precision=error_precision)


def conv_rows(padded, kernel):
    tile_rows = padded.shape[0] - 2
    channels = padded.shape[2]
    total = jnp.zeros((tile_rows * padded.shape[1], kernel.shape[3]), jnp.float32)
    for row_off in range(3):
        row_band = padded[row_off:row_off + tile_rows]
        for col_off in range(3):
            shifted = jnp.roll(row_band, 1 - col_off, axis=1)
            total = total + jnp.dot(shifted.reshape(-1, channels), kernel[row_off, col_off], preferred_element_type=jnp.float32)
    return total.reshape(tile_rows, padded.shape[1], kernel.shape[3])


def pad_rows(field_in):
    return jnp.pad(field_in, ((1, 1), (0, 0), (0, 0)))


def flipped(kernel):
    return kernel[::-1, ::-1].transpose(0, 1, 3, 2)


def reference(state, background, back_precision, conv_first, bias_first, conv_second, sounding_tile, sounding_cells, cell_weights, observations, live_counts, layer_in, bias_in, layer_out, bias_out, error_precision):
    state_bf = state.astype(jnp.bfloat16)
    hidden = jnp.tanh(conv_rows(pad_rows(state_bf), conv_first) + bias_first).astype(jnp.bfloat16)
    observed = (state + conv_rows(pad_rows(hidden), conv_second)).astype(jnp.bfloat16)
    observed_flat = observed.reshape(-1, CH)
    flat_index = (sounding_tile * (ROWS_DEV * NCOLS) + sounding_cells).astype(jnp.int32)
    positions = jnp.arange(SOUNDINGS, dtype=jnp.int32)
    live_mask = ((positions % SND_DEV) < jnp.repeat(live_counts, SND_DEV)).astype(jnp.float32)

    def one_block(bundle):
        indices, weights, measured, alive = bundle
        picked = observed_flat[indices].astype(jnp.float32)
        interpolated = jnp.sum(picked * weights[:, :, None], axis=1).astype(jnp.bfloat16)
        pre_act = jnp.dot(interpolated, layer_in, preferred_element_type=jnp.float32) + bias_in
        activated = jnp.tanh(pre_act).astype(jnp.bfloat16)
        radiance = jnp.dot(activated, layer_out, preferred_element_type=jnp.float32) + bias_out
        innovation = (radiance - measured) * alive[:, None]
        weighted = jnp.dot(innovation, error_precision, precision=lax.Precision.HIGHEST)
        back_act = jnp.dot(weighted.astype(jnp.bfloat16), layer_out.T, preferred_element_type=jnp.float32)
        act_wide = activated.astype(jnp.float32)
        pre_grad = (back_act * (1.0 - act_wide * act_wide)).astype(jnp.bfloat16)
        return jnp.dot(pre_grad, layer_in.T, preferred_element_type=jnp.float32)

    sounding_grad = lax.map(one_block, (
        flat_index.reshape(N_DEV, SND_DEV, MARGIN),
        cell_weights.reshape(N_DEV, SND_DEV, MARGIN),
        observations.reshape(N_DEV, SND_DEV, NCHAN),
        live_mask.reshape(N_DEV, SND_DEV))).reshape(SOUNDINGS, CH)
    ref_terms = cell_weights[:, :, None] * sounding_grad[:, None, :]
    obs_grad = jnp.zeros((NROWS * NCOLS, CH), jnp.float32).at[flat_index.reshape(-1)].add(ref_terms.reshape(-1, CH))
    obs_grad = obs_grad.reshape(state.shape)
    hid_grad = conv_rows(pad_rows(obs_grad.astype(jnp.bfloat16)), flipped(conv_second))
    hidden_wide = hidden.astype(jnp.float32)
    act_grad = (hid_grad * (1.0 - hidden_wide * hidden_wide)).astype(jnp.bfloat16)
    model_grad = conv_rows(pad_rows(act_grad), flipped(conv_first))
    return obs_grad + model_grad + back_precision * (state - background)
```

```python
import functools

import jax
import jax.numpy as jnp
from jax import lax
from jax.experimental import pallas as pl
from jax.experimental.pallas import tpu as pltpu
from jax.sharding import PartitionSpec as P

F32 = jnp.float32
BF16 = jnp.bfloat16
MESH = pl.DeviceIdType.MESH
LANES = 128


def dot(a, b):
    return jnp.dot(a, b, preferred_element_type=F32)


def dot_nt(a, b):
    return lax.dot_general(a, b, (((1,), (1,)), ((), ())), preferred_element_type=F32)


def kernel(
    n,
    table_ref,
    live_ref,
    back_precision_ref,
    bias_first_ref,
    bias_in_ref,
    bias_out_ref,
    state_hbm,
    background_hbm,
    conv_first_hbm,
    conv_second_hbm,
    observations_hbm,
    layer_in_hbm,
    layer_out_hbm,
    precision_hbm,
    out_ref,
    state_ref,
    background_ref,
    conv_first_ref,
    conv_second_ref,
    adj_first_ref,
    adj_second_ref,
    observations_ref,
    layer_in_ref,
    layer_out_ref,
    precision_ref,
    field_ref,
    halo_ref,
    taps_ref,
    hidden_ref,
    hidden_taps_ref,
    observed_t_ref,
    place_ref,
    place_t_ref,
    share_t_ref,
    grad_ref,
    req_src,
    req_dst,
    ret_src,
    ret_dst,
    out_src,
    out_dst,
    load_sem,
    halo_send,
    halo_recv,
    req_send,
    req_recv,
    ret_send,
    ret_recv,
    out_send,
    out_recv,
):
    me = lax.axis_index("dev")
    rows, cols, ch = state_ref.shape
    slots = place_t_ref.shape[0]
    listed = place_t_ref.shape[1]
    cap = slots // n
    per = LANES // cap
    groups = slots // LANES
    up = lax.rem(me + n - 1, n)
    down = lax.rem(me + 1, n)

    loads = [
        pltpu.make_async_copy(src, dst, load_sem.at[i])
        for i, (src, dst) in enumerate(
            (
                (state_hbm, state_ref),
                (conv_first_hbm, conv_first_ref),
                (conv_second_hbm, conv_second_ref),
                (layer_in_hbm, layer_in_ref),
                (layer_out_hbm, layer_out_ref),
                (observations_hbm, observations_ref),
                (precision_hbm, precision_ref),
                (background_hbm, background_ref),
            )
        )
    ]
    for load in loads:
        load.start()

    barrier = pltpu.get_barrier_semaphore()

    def greet(k, carry):
        pl.semaphore_signal(
            barrier, inc=1, device_id=(lax.rem(me + k, n),), device_id_type=MESH
        )
        return carry

    lax.fori_loop(1, n, greet, 0)

    def exchange(src, dst, send, recv):
        def start(k, carry):
            target = lax.rem(me + k, n)
            pltpu.make_async_remote_copy(
                src_ref=src.at[target],
                dst_ref=dst.at[me],
                send_sem=send.at[k],
                recv_sem=recv.at[k],
                device_id=(target,),
                device_id_type=MESH,
            ).start()
            return carry

        lax.fori_loop(1, n, start, 0)

    def settle(src, dst, send, recv):
        def wait(k, carry):
            copy = pltpu.make_async_remote_copy(
                src_ref=src.at[lax.rem(me + k, n)],
                dst_ref=dst.at[lax.rem(me + n - k, n)],
                send_sem=send.at[k],
                recv_sem=recv.at[k],
                device_id=(lax.rem(me + k, n),),
                device_id_type=MESH,
            )
            copy.wait_recv()
            copy.wait_send()
            return carry

        lax.fori_loop(1, n, wait, 0)

    def rim(phase):
        return [
            pltpu.make_async_remote_copy(
                src_ref=field_ref.at[phase, pl.ds(rows - 2 if side == 0 else 0, 2)],
                dst_ref=halo_ref.at[phase, side],
                send_sem=halo_send.at[phase, side],
                recv_sem=halo_recv.at[phase, side],
                device_id=(down if side == 0 else up,),
                device_id_type=MESH,
            )
            for side in range(2)
        ]

    def put_taps(taps, row, value):
        taps[row, :, pl.ds(0, ch)] = pltpu.roll(value, 1, 0).astype(BF16)
        taps[row, :, pl.ds(ch, ch)] = value.astype(BF16)
        taps[row, :, pl.ds(2 * ch, ch)] = pltpu.roll(value, cols - 1, 0).astype(BF16)

    def conv_row(taps, row, weights):
        return (
            dot(taps[row], weights[0])
            + dot(taps[row + 1], weights[1])
            + dot(taps[row + 2], weights[2])
        )

    def put_halo(phase):
        for side in range(2):
            inside = (me > 0) if side == 0 else (me < n - 1)
            for i in range(2):
                value = halo_ref[phase, side, i].astype(F32) * inside.astype(F32)
                put_taps(taps_ref, i if side == 0 else rows + 2 + i, value)

    def within(row):
        first, last = me == 0, me == n - 1
        return 1.0 - jnp.where(
            (first & (row == 0)) | (last & (row == rows + 1)), 1.0, 0.0
        ).astype(F32)

    loads[0].wait()

    def take_state(r, carry):
        field_ref[0, r] = state_ref[r].astype(BF16)
        return carry

    lax.fori_loop(0, rows, take_state, 0)

    table = table_ref[...]
    tile_row = table[8:9]
    tile_col = jnp.broadcast_to(tile_row, (LANES, listed)).T[:, 0:1]
    same = tile_col == tile_row
    from_col = lax.broadcasted_iota(jnp.int32, (listed, listed), 0)
    from_row = lax.broadcasted_iota(jnp.int32, (listed, listed), 1)
    rank_row = jnp.sum(jnp.where(same & (from_col < from_row), 1.0, 0.0), axis=0, keepdims=True)
    rank_col = jnp.sum(jnp.where(same & (from_row < from_col), 1.0, 0.0), axis=1, keepdims=True)
    slot_row = (tile_row * cap + rank_row).astype(jnp.int32)
    slot_col = (tile_col * cap + rank_col).astype(jnp.int32)
    for g in range(groups):
        rowid = lax.broadcasted_iota(jnp.int32, (LANES, listed), 0) + g * LANES
        place_t_ref[pl.ds(g * LANES, LANES)] = jnp.where(rowid == slot_row, 1.0, 0.0).astype(BF16)
        colid = lax.broadcasted_iota(jnp.int32, (listed, LANES), 1) + g * LANES
        place_ref[:, pl.ds(g * LANES, LANES)] = jnp.where(colid == slot_col, 1.0, 0.0).astype(BF16)

    values = table[0:8]
    part_1 = values.astype(BF16).astype(F32)
    part_2 = (values - part_1).astype(BF16).astype(F32)
    part_3 = values - part_1 - part_2
    parts = jnp.concatenate([part_1, part_2, part_3, jnp.zeros_like(values)], axis=0).astype(BF16)
    own_lanes = lax.broadcasted_iota(jnp.int32, (8, LANES), 1) // cap == lax.rem(me, per)
    for g in range(groups):
        spread = dot_nt(parts, place_t_ref[pl.ds(g * LANES, LANES)])
        spread = spread[0:8] + spread[8:16] + spread[16:24]
        for i in range(per):
            turned = pltpu.roll(spread, lax.rem(lax.rem(me, per) + per - i, per) * cap, 1)
            req_src[g * per + i] = jnp.where(own_lanes, turned, 0.0)
    req_dst[me] = req_src[me]

    pl.semaphore_wait(barrier, n - 1)
    forward_rim = rim(0)
    for copy in forward_rim:
        copy.start()
    exchange(req_src, req_dst, req_send, req_recv)

    def take_taps(r, carry):
        put_taps(taps_ref, r + 2, state_ref[r].astype(BF16).astype(F32))
        return carry

    lax.fori_loop(0, rows, take_taps, 0)
    loads[1].wait()
    loads[2].wait()
    for kernel_ref, adj_ref in ((conv_first_ref, adj_first_ref), (conv_second_ref, adj_second_ref)):
        for a in range(3):
            for b in range(3):
                tap = kernel_ref[2 - a, pl.ds((2 - b) * ch, ch)].astype(F32)
                adj_ref[a, pl.ds(b * ch, ch)] = tap.T.astype(BF16)

    def forward_row(row, carry):
        value = jnp.tanh(conv_row(taps_ref, row, conv_first_ref) + bias_first_ref[...])
        value = value.astype(BF16).astype(F32) * within(row)
        hidden_ref[row] = value
        put_taps(hidden_taps_ref, row, value)
        return carry

    lax.fori_loop(2, rows, forward_row, 0)
    for copy in forward_rim:
        copy.wait_recv()
    put_halo(0)
    lax.fori_loop(0, 2, forward_row, 0)
    lax.fori_loop(rows, rows + 2, forward_row, 0)

    def observed_row(r, carry):
        value = state_ref[r] + conv_row(hidden_taps_ref, r, conv_second_ref)
        observed_t_ref[:, pl.ds(pl.multiple_of(r * cols, LANES), cols)] = value.T.astype(BF16)
        return carry

    lax.fori_loop(0, rows, observed_row, 0)

    settle(req_src, req_dst, req_send, req_recv)
    wanted = []
    for g in range(groups):
        total = req_dst[g * per]
        for i in range(1, per):
            total = total + req_dst[g * per + i]
        wanted.append(total)
    margin = 4

    def build_shares(c, carry):
        base = pl.multiple_of(c * LANES, LANES)
        cell = (lax.broadcasted_iota(jnp.int32, (LANES, LANES), 0) + base).astype(F32)
        for g in range(groups):
            total = jnp.zeros((LANES, LANES), F32)
            for k in range(margin):
                total = total + jnp.where(
                    cell == wanted[g][k : k + 1], wanted[g][margin + k : margin + k + 1], 0.0
                )
            share_t_ref[pl.ds(base, LANES), pl.ds(g * LANES, LANES)] = total.astype(BF16)
        return carry

    lax.fori_loop(0, rows * cols // LANES, build_shares, 0)

    def blend(g, carry):
        width = 2 * LANES
        base = pl.multiple_of(g * width, width)
        blended = dot(observed_t_ref[...], share_t_ref[:, pl.ds(base, width)]).T
        ret_src[pl.ds(g * (width // cap), width // cap)] = blended.reshape(
            width // cap, cap, ch
        ).astype(BF16)
        return carry

    lax.fori_loop(0, groups // 2, blend, 0)
    ret_dst[me] = ret_src[me]
    exchange(ret_src, ret_dst, ret_send, ret_recv)
    for load in loads[3:7]:
        load.wait()
    precision = precision_ref[...].astype(BF16)
    settle(ret_src, ret_dst, ret_send, ret_recv)
    returned = ret_dst[...].astype(F32).reshape(slots, ch).astype(BF16)
    live = live_ref[0]
    block = listed // 4
    for s in range(0, listed, block):
        span = pl.ds(s, block)
        interpolated = dot(place_ref[span], returned).astype(BF16)
        activated = jnp.tanh(dot(interpolated, layer_in_ref[...]) + bias_in_ref[...]).astype(BF16)
        radiance = dot(activated, layer_out_ref[...]) + bias_out_ref[...]
        alive = lax.broadcasted_iota(jnp.int32, (block, 1), 0) + s < live
        innovation = jnp.where(alive, radiance - observations_ref[span], 0.0)
        weighted = dot(innovation.astype(BF16), precision)
        back_act = dot_nt(weighted.astype(BF16), layer_out_ref[...])
        act_wide = activated.astype(F32)
        pre_grad = (back_act * (1.0 - act_wide * act_wide)).astype(BF16)
        grad_ref[span] = dot_nt(pre_grad, layer_in_ref[...]).astype(BF16)

    def dispatch(g, carry):
        width = 2 * LANES
        base = pl.multiple_of(g * width, width)
        outgoing = dot(place_t_ref[pl.ds(base, width)], grad_ref[...])
        out_src[pl.ds(g * (width // cap), width // cap)] = outgoing.reshape(
            width // cap, cap, ch
        ).astype(BF16)
        return carry

    lax.fori_loop(0, groups // 2, dispatch, 0)
    out_dst[me] = out_src[me]
    exchange(out_src, out_dst, out_send, out_recv)
    settle(out_src, out_dst, out_send, out_recv)
    arrived = out_dst[...].astype(F32).reshape(slots, ch).astype(BF16)

    def gather_grad(r, carry):
        value = dot(share_t_ref[pl.ds(pl.multiple_of(r * cols, LANES), cols)], arrived)
        out_ref[r] = value
        field_ref[1, r] = value.astype(BF16)
        return carry

    lax.fori_loop(0, rows, gather_grad, 0)
    for copy in forward_rim:
        copy.wait_send()
    backward_rim = rim(1)
    for copy in backward_rim:
        copy.start()

    def take_grad(r, carry):
        put_taps(taps_ref, r + 2, out_ref[r].astype(BF16).astype(F32))
        return carry

    lax.fori_loop(0, rows, take_grad, 0)

    def backward_row(row, carry):
        value = conv_row(taps_ref, row, adj_second_ref)
        hidden = hidden_ref[row]
        value = value * (1.0 - hidden * hidden) * within(row)
        put_taps(hidden_taps_ref, row, value.astype(BF16).astype(F32))
        return carry

    lax.fori_loop(2, rows, backward_row, 0)
    for copy in backward_rim:
        copy.wait_recv()
    put_halo(1)
    lax.fori_loop(0, 2, backward_row, 0)
    lax.fori_loop(rows, rows + 2, backward_row, 0)
    loads[7].wait()

    def last_row(r, carry):
        out_ref[r] = (
            out_ref[r]
            + conv_row(hidden_taps_ref, r, adj_first_ref)
            + back_precision_ref[...] * (state_ref[r] - background_ref[r])
        )
        return carry

    lax.fori_loop(0, rows, last_row, 0)
    for copy in backward_rim:
        copy.wait_send()


def per_device(
    state,
    background,
    back_precision,
    conv_first,
    bias_first,
    conv_second,
    sounding_tile,
    sounding_cells,
    cell_weights,
    observations,
    live_counts,
    layer_in,
    bias_in,
    layer_out,
    bias_out,
    error_precision,
):
    rows, cols, ch = state.shape
    n = lax.axis_size("dev")
    listed = sounding_tile.shape[0]
    slots = 2 * listed
    cap = slots // n
    hid, chan = layer_out.shape
    table = jnp.concatenate(
        [
            sounding_cells.T.astype(F32),
            cell_weights.T,
            jnp.broadcast_to(sounding_tile.reshape(1, listed).astype(F32), (8, listed)),
        ],
        axis=0,
    )
    vmem = pl.BlockSpec(memory_space=pltpu.VMEM)
    hbm = pl.BlockSpec(memory_space=pl.ANY)
    dma = pltpu.SemaphoreType.DMA
    return pl.pallas_call(
        functools.partial(kernel, n),
        out_shape=jax.ShapeDtypeStruct(state.shape, F32),
        in_specs=[vmem, pl.BlockSpec(memory_space=pltpu.SMEM)] + [vmem] * 4 + [hbm] * 8,
        out_specs=vmem,
        scratch_shapes=[
            pltpu.VMEM(state.shape, F32),
            pltpu.VMEM(state.shape, F32),
            pltpu.VMEM((3, 3 * ch, ch), BF16),
            pltpu.VMEM((3, 3 * ch, ch), BF16),
            pltpu.VMEM((3, 3 * ch, ch), BF16),
            pltpu.VMEM((3, 3 * ch, ch), BF16),
            pltpu.VMEM((listed, chan), F32),
            pltpu.VMEM((ch, hid), BF16),
            pltpu.VMEM((hid, chan), BF16),
            pltpu.VMEM((chan, chan), F32),
            pltpu.VMEM((2, rows, cols, ch), BF16),
            pltpu.VMEM((2, 2, 2, cols, ch), BF16),
            pltpu.VMEM((rows + 4, cols, 3 * ch), BF16),
            pltpu.VMEM((rows + 2, cols, ch), F32),
            pltpu.VMEM((rows + 2, cols, 3 * ch), BF16),
            pltpu.VMEM((ch, rows * cols), BF16),
            pltpu.VMEM((listed, slots), BF16),
            pltpu.VMEM((slots, listed), BF16),
            pltpu.VMEM((rows * cols, slots), BF16),
            pltpu.VMEM((listed, ch), BF16),
            pltpu.VMEM((n, 8, LANES), F32),
            pltpu.VMEM((n, 8, LANES), F32),
            pltpu.VMEM((n, cap, ch), BF16),
            pltpu.VMEM((n, cap, ch), BF16),
            pltpu.VMEM((n, cap, ch), BF16),
            pltpu.VMEM((n, cap, ch), BF16),
            dma((8,)),
            dma((2, 2)),
            dma((2, 2)),
            dma((n,)),
            dma((n,)),
            dma((n,)),
            dma((n,)),
            dma((n,)),
            dma((n,)),
        ],
        compiler_params=pltpu.CompilerParams(
            collective_id=0, has_side_effects=True, vmem_limit_bytes=60 * 1024 * 1024
        ),
        name="step",
    )(
        table,
        live_counts,
        back_precision.reshape(1, -1),
        bias_first.reshape(1, -1),
        bias_in.reshape(1, -1),
        bias_out.reshape(1, -1),
        state,
        background,
        conv_first.reshape(3, 3 * ch, ch),
        conv_second.reshape(3, 3 * ch, ch),
        observations,
        layer_in,
        layer_out,
        error_precision,
    )


def solution(mesh):
    return jax.shard_map(
        per_device,
        mesh=mesh,
        in_specs=(
            P("dev", None, None),
            P("dev", None, None),
            P(),
            P(),
            P(),
            P(),
            P("dev", None),
            P("dev", None),
            P("dev", None),
            P("dev", None),
            P("dev"),
            P(),
            P(),
            P(),
            P(),
            P(),
        ),
        out_specs=P("dev", None, None),
        check_vma=False,
    )
```
